128 devices in a mesh: mem: 16 (over y, x), pix: 8 (over z, core).
Axes of the slice: x: 4, y: 4, z: 4, core: 2. Of those that a mesh axis runs over, the one named last changes fastest.
Arguments:
- prior_motion: bfloat16 [64, 16, 262144], P('mem', None, 'pix'), may hold values from -6 to 6
- measured_motion: float32 [1200], replicated, may hold values from -1.6 to 1.6
- measurement_noise_stddev: float32 [1200], replicated, may hold values from 0.05 to 0.5
- gaussian_jitter: float32 [2, 1200, 64], replicated, may hold values from -6 to 6
- scene_couples: int32 [2, 1200], replicated, may hold values from 0 to 15, as said below
- targeted_tile_number: int32 [1200], replicated, may hold values from 0 to 4095
Outputs:
- analysis: bfloat16 [64, 16, 262144], P('mem', None, 'pix')
The draws below stay inside these ranges and needn't reach their ends.
Inputs may be any that keep to these rules, and one draw needn't show every extreme that they name: scene_couples[0, k] < scene_couples[1, k]: row 0 holds the earlier acquisition, row 1 the later.
All inputs are finite; a program needn't handle non-finite values.
Results may differ from the reference program's by a relative error of at most 0.011.
Values may be sent and summed in bfloat16 or wider, within the bound.
No kernel may reach another device: no remote copies, remote signals or barrier semaphores. Data moves between devices by JAX's collectives and lax.ppermute only.
A program may use at most 128 MiB of HBM per device.

```python
import math
import jax
import jax.numpy as jnp
from jax import lax

REALIZATION_NUM = 64
SCENE_TIMES = 16
NOBS = 1200
BLK = 64
PASS_COUNT = 2
RASTER_CELLS = 262144
NBLK = 4096
N_MEM = 16
N_PIX = 8


def draw_scene_couples(key, part):
    key_first = jax.random.fold_in(key, 11)
    key_gap = jax.random.fold_in(key, 12)
    earlier = jax.random.randint(key_first, (NOBS,), 0, SCENE_TIMES - 1)
    offset = jax.random.randint(key_gap, (NOBS,), 0, SCENE_TIMES - 1)
    later = earlier + 1 + offset % (SCENE_TIMES - 1 - earlier)
    return jnp.stack([earlier, later]).astype(jnp.int32)


def plant(entries, rng, least, largest):
    extent = entries.shape
    index_at = [jax.random.randint(jax.random.fold_in(rng, axis), (), 0, extent[axis]) for axis in range(len(extent))]
    entries = entries.at[tuple(index_at)].set(least)
    longest = extent.index(max(extent))
    index_at[longest] = (index_at[longest] + 1) % extent[longest]
    return entries.at[tuple(index_at)].set(largest)


def level_of(key, extent, split, low, top_value):
    factor_of, own = 1.0, jax.random.fold_in(key, 6)
    for position, blocks in split:
        draws = jnp.exp(jax.random.uniform(jax.random.fold_in(own, position), (blocks,), jnp.float32, low / len(split), top_value / len(split)))
        factor_of = factor_of * jnp.repeat(draws, extent[position] // blocks).reshape([-1 if axis == position else 1 for axis in range(len(extent))])
    return factor_of


def noise(key, shape, width, most, split=(), kind=jnp.bfloat16):
    entries = jax.random.normal(key, shape, jnp.float32) * width
    if len(split) > 0:
        entries = level_of(key, shape, split, -0.22, 0.18) * entries
    return jnp.clip(entries, min=-most, max=most).astype(kind)


def setup_inputs(seed: int = 0) -> dict:
    arg_keys = jax.random.split(jax.random.key(seed), 7)
    prior_motion = noise(arg_keys[0], (REALIZATION_NUM, SCENE_TIMES, RASTER_CELLS), 1.0, 6.0, ((0, 16), (2, 8)))
    measured_motion = noise(arg_keys[1], (NOBS,), 0.2, 1.6, (), jnp.float32)
    measurement_noise_stddev = jnp.clip(jnp.exp(jax.random.uniform(arg_keys[2], (NOBS,), jnp.float32, math.log(0.05), math.log(0.5))), 0.05, 0.5)
    gaussian_jitter = noise(arg_keys[3], (PASS_COUNT, NOBS, REALIZATION_NUM), 1.0, 6.0, (), jnp.float32)
    scene_couples = draw_scene_couples(jax.random.fold_in(arg_keys[6], 71), 0)
    targeted_tile_number = plant(jax.random.randint(arg_keys[5], (NOBS,), 0, NBLK), jax.random.fold_in(arg_keys[5], 1), 0, NBLK - 1).astype(jnp.int32)
    return {"prior_motion": prior_motion, "measured_motion": measured_motion, "measurement_noise_stddev": measurement_noise_stddev, "gaussian_jitter": gaussian_jitter, "scene_couples": scene_couples, "targeted_tile_number": targeted_tile_number}


def update_tile(tile_state, mixing):
    realization_vectors = tile_state.shape[0]
    average = lax.optimization_barrier(jnp.sum(tile_state, axis=0, dtype=jnp.float32)) / realization_vectors
    anomaly = (tile_state.astype(jnp.float32) - average).astype(jnp.bfloat16)
    change = jnp.dot(mixing.T.astype(jnp.float32), anomaly.reshape(realization_vectors, -1).astype(jnp.float32), preferred_element_type=jnp.float32)
    return (tile_state.astype(jnp.float32) + change.reshape(tile_state.shape)).astype(jnp.bfloat16)

def reference(prior_motion, measured_motion, measurement_noise_stddev, gaussian_jitter, scene_couples, targeted_tile_number):
    realization_vectors = prior_motion.shape[0]
    spread_factor = float(PASS_COUNT)
    member_anomaly = jnp.sqrt(jnp.float32(spread_factor)) * measurement_noise_stddev
    ground_motion_vector = prior_motion
    for iteration in range(PASS_COUNT):
        sums = lax.optimization_barrier(jnp.sum(ground_motion_vector.reshape(realization_vectors, SCENE_TIMES, NBLK, BLK), axis=3, dtype=jnp.float32))
        predicted = ((sums[:, scene_couples[1], targeted_tile_number] - sums[:, scene_couples[0], targeted_tile_number]) / BLK).T
        centred = predicted - lax.optimization_barrier(jnp.mean(predicted, axis=1, keepdims=True))
        scaled = centred / (member_anomaly[:, None] * math.sqrt(realization_vectors - 1))
        misfit = (measured_motion[:, None] + member_anomaly[:, None] * gaussian_jitter[iteration] - predicted) / member_anomaly[:, None]
        gram = jnp.dot(scaled.T.astype(jnp.float32), scaled.astype(jnp.float32), precision=lax.Precision.HIGHEST, preferred_element_type=jnp.float32)
        cross = jnp.dot(scaled.T.astype(jnp.float32), misfit.astype(jnp.float32), precision=lax.Precision.HIGHEST, preferred_element_type=jnp.float32)
        factor = jnp.linalg.cholesky(jnp.eye(realization_vectors, dtype=jnp.float32) + gram)
        mixing = (jax.scipy.linalg.cho_solve((factor, True), cross) / math.sqrt(realization_vectors - 1)).astype(jnp.bfloat16)
        tiles = jnp.moveaxis(ground_motion_vector.reshape(realization_vectors, SCENE_TIMES, N_PIX * N_MEM, -1), 2, 0)

        def one_tile(tile_state):
            return update_tile(tile_state, mixing)
        fresh = lax.map(one_tile, tiles)
        ground_motion_vector = jnp.moveaxis(fresh, 0, 2).reshape(ground_motion_vector.shape)
    return ground_motion_vector
```

```python
import math

import jax
import jax.numpy as jnp
from jax import lax
from jax.sharding import PartitionSpec as P

BLK = 64
PASS_COUNT = 2
HI = lax.Precision.HIGHEST


def mm(a, b):
    return jnp.dot(a, b, precision=HI, preferred_element_type=jnp.float32)


def tn(a, b):
    return lax.dot_general(
        a, b, (((0,), (0,)), ((), ())), precision=HI, preferred_element_type=jnp.float32
    )


def local_sums(parts):
    n_part, members, dates, width = parts.shape
    blocks = width // BLK
    summer = (
        jnp.arange(width, dtype=jnp.int32)[:, None] // BLK
        == jnp.arange(blocks, dtype=jnp.int32)[None, :]
    ).astype(jnp.bfloat16)
    flat = jnp.dot(parts.reshape(-1, width), summer, preferred_element_type=jnp.float32)
    flat = flat.reshape(n_part, members * dates, blocks)
    return jnp.moveaxis(flat, 0, 1).reshape(members * dates, n_part * blocks)


def local_predicted(sums, dates, first_block, scene_couples, targeted_tile_number):
    blocks = sums.shape[1]
    block_range = first_block + jnp.arange(blocks, dtype=jnp.int32)
    block_table = (block_range[:, None] == targeted_tile_number[None, :]).astype(jnp.float32)
    picked = mm(sums, block_table)
    timeline = jnp.arange(dates, dtype=jnp.int32)
    pair_table = (timeline[:, None] == scene_couples[1][None, :]).astype(jnp.float32) - (
        timeline[:, None] == scene_couples[0][None, :]
    ).astype(jnp.float32)
    picked = picked.reshape(-1, dates, picked.shape[1])
    return jnp.sum(picked * pair_table[None], axis=1) / BLK


def solve(gram, cross):
    n = gram.shape[0]
    factor = jnp.linalg.cholesky(jnp.eye(n, dtype=jnp.float32) + gram)
    mixing = jax.scipy.linalg.cho_solve((factor, True), cross) / math.sqrt(n - 1)
    return mixing.astype(jnp.bfloat16).astype(jnp.float32)


def combined_mixing(gram, cross_first, cross_second):
    n = gram.shape[0]
    first = solve(gram, cross_first)
    moved = first + jnp.eye(n, dtype=jnp.float32)
    moved = moved - jnp.mean(moved, axis=1, keepdims=True)
    gram_moved = mm(gram, moved)
    gram_next = tn(moved, gram_moved)
    cross_next = tn(moved, cross_second - math.sqrt(n - 1) * mm(gram, first))
    second = solve(gram_next, cross_next)
    whole = first + mm(moved, second)
    return whole - jnp.mean(whole, axis=0, keepdims=True)


def body(
    prior_motion,
    measured_motion,
    measurement_noise_stddev,
    gaussian_jitter,
    scene_couples,
    targeted_tile_number,
):
    members, dates, cells = prior_motion.shape
    n_mem = lax.axis_size("mem")
    width = cells // n_mem
    n = members * n_mem
    parts = jnp.moveaxis(prior_motion.reshape(members, dates, n_mem, width), 2, 0)
    state = lax.all_to_all(parts, "mem", split_axis=0, concat_axis=0, tiled=True)

    first_block = lax.axis_index("pix") * (cells // BLK)
    predicted = local_predicted(
        local_sums(parts), dates, first_block, scene_couples, targeted_tile_number
    )
    predicted = lax.all_gather(predicted, "mem", axis=0, tiled=True)
    in_tile = (targeted_tile_number // (cells // BLK)) == lax.axis_index("pix")
    spread = jnp.sqrt(jnp.float32(float(PASS_COUNT))) * measurement_noise_stddev
    scaled = (predicted - jnp.mean(predicted, axis=0, keepdims=True)) / (
        spread * math.sqrt(n - 1)
    )[None, :]
    fixed = (measured_motion[None, :] - predicted) / spread[None, :]
    misfits = [
        jnp.where(in_tile[None, :], fixed + gaussian_jitter[i].T, 0.0) for i in range(PASS_COUNT)
    ]
    right = jnp.concatenate([scaled] + misfits, axis=0)
    products = lax.dot_general(
        scaled, right, (((1,), (1,)), ((), ())), precision=HI, preferred_element_type=jnp.float32
    )
    products = lax.psum(products, "pix")
    mixing = combined_mixing(products[:, :n], products[:, n : 2 * n], products[:, 2 * n :])
    mixing = mixing.astype(jnp.bfloat16)

    rows = n * dates
    spread_mixing = (
        mixing.T[:, None, :, None] * jnp.eye(dates, dtype=jnp.bfloat16)[None, :, None, :]
    ).reshape(rows, rows)
    flat = state.reshape(rows, width)
    change = jnp.dot(spread_mixing, flat, preferred_element_type=jnp.float32)
    fresh = (flat.astype(jnp.float32) + change).astype(jnp.bfloat16)
    fresh = fresh.reshape(n_mem, members, dates, width)
    back = lax.all_to_all(fresh, "mem", split_axis=0, concat_axis=0, tiled=True)
    return jnp.moveaxis(back, 0, 2).reshape(members, dates, cells)


def solution(mesh):
    return jax.shard_map(
        body,
        mesh=mesh,
        in_specs=(P("mem", None, "pix"), P(), P(), P(), P(), P()),
        out_specs=P("mem", None, "pix"),
        check_vma=False,
    )
```
